32 devices in a mesh: groups: 2 (over y), sky: 4 (over z), epoch: 2 (over x), band: 2 (over core).
Axes of the slice: x: 2, y: 2, z: 4, core: 2. Of those that a mesh axis runs over, the one named last changes fastest.
Arguments:
- slot_pixels: bfloat16 [96, 6, 32, 512], P(('groups', 'sky', 'epoch'), 'band'), parts along dimension 0, may hold values from -6 to 6
- slot_tile: int32 [96, 1], P(('groups', 'sky', 'epoch')), parts along dimension 0, may hold values from 0 to 3; in each aligned block of 6 rows (0 to 5, 6 to 11, ...) at most 2 rows name the same one
- slot_offset: int32 [96, 2], P(('groups', 'sky', 'epoch')), parts along dimension 0, may hold values from -5 to 5
- slot_frac: bfloat16 [96, 2], P(('groups', 'sky', 'epoch')), parts along dimension 0, may hold values from 0.049804688 to 0.94921875
- slot_sigma: bfloat16 [96, 6], P(('groups', 'sky', 'epoch'), 'band'), parts along dimension 0, may hold values from 0.5 to 2
- clip_mask: int32 [96, 6, 16], P(('groups', 'sky', 'epoch')), parts along dimension 0, may hold values 0 or 1
- slot_count: int32 [16], P(('groups', 'sky', 'epoch')), parts along dimension 0, may hold values from 4 to 6
- template: bfloat16 [6, 256, 512], P('band', ('groups', 'sky')), parts along dimension 1, may hold values from -6 to 6
- prior_weight: float32 [6, 256], P('band', ('groups', 'sky')), parts along dimension 1, may hold values from 0.5 to 4
Outputs:
- coadd_image: bfloat16 [6, 256, 512], P('band', ('groups', 'sky'), 'epoch'), parts along dimension 1
- depth_norm: bfloat16 [6, 256, 512], P('band', ('groups', 'sky'), 'epoch'), parts along dimension 1
The draws below stay inside these ranges and needn't reach their ends.
There are 2 independent parts, one for each index of `groups`. The reference program is written for one: setup_inputs(seed, part) draws one part's arguments, and reference() takes and returns one part's arrays. A program takes and returns all parts, laid end to end along the dimension named above; each array names one. Nothing has to cross between parts.
Inputs may be any that keep to these rules, and one draw needn't show every extreme that they name: `slot_tile`: among the 6 rows of one reading device no owner is named more than 2 times, a bound that some block reaches. `slot_count`: slots of a reading device at or after its count are padding.
All inputs are finite; a program needn't handle non-finite values. No bound on the sum of `clip_mask` on one device may be relied on, other than what follows from the above.
Results may differ from the reference program's by a relative error of at most 0.014.
Values may be sent and summed in bfloat16 or wider, within the bound.
A program may use at most 64 MiB of HBM per device.

```python
import math
import jax
import jax.numpy as jnp
import numpy as np
from jax import lax

BAND_COUNT = 6
TILE_COLS = 512
ROWS_DEV = 32
MAX_SHIFT = 5
MARGIN = 8
CAPACITY = 2
SLOT_DEV = 6
SLOT_TOTAL = 48
PATCH_ROWS = 128
N_SKY = 4
N_EPOCH = 2


def plant(array, key, least, high):
    longest = array.shape.index(max(array.shape))
    spots = []
    for shift in (0, 1):
        where = [jax.random.randint(jax.random.fold_in(key, axis), (), 0, length) for axis, length in enumerate(array.shape)]
        where[longest] = (where[longest] + shift) % array.shape[longest]
        spots.append(tuple(where))
    return array.at[spots[0]].set(least).at[spots[1]].set(high)


def block_levels(own_key, extent, shards, smallest, high):
    level = 1.0
    for position, parts in shards:
        steps = jax.random.uniform(jax.random.fold_in(jax.random.fold_in(own_key, 6), position), (parts,), jnp.float32, smallest / len(shards), high / len(shards))
        level = level * jnp.repeat(jnp.exp(steps), extent[position] // parts).reshape((-1,) + (1,) * (len(extent) - 1 - position))
    return level


def shared_out(stream_key, own, number, rows, amount, top, most, skew):
    sequence = jax.random.permutation(stream_key, amount)
    heavy_load, usual = portions_of(amount, rows * top, most, skew, True), portions_of(amount, rows * top, most, skew, False)
    places = jnp.arange(amount)

    def named(lengths, offset_by):
        used = int((lengths > 0).sum())
        fixed = max(1, used // 4)
        moved = fixed + (places - fixed + offset_by * (used - fixed)) % max(1, amount - fixed)
        return jnp.zeros((amount,), jnp.int32).at[sequence[jnp.where(places < fixed, places, moved)]].set(jnp.asarray(lengths, jnp.int32))

    lengths = jnp.where(number % 4 == 0, named(heavy_load, number // 4), named(usual, number - number // 4 - 1))
    mixed = jax.random.permutation(jax.random.fold_in(own, 3), amount)
    giver, receiver = mixed[0:amount // 2 * 2:2], mixed[1:amount // 2 * 2:2]
    slack = jnp.minimum(lengths[giver] - 1, most - lengths[receiver]) // 2
    slack = jnp.where((giver == sequence[0]) | (receiver == sequence[0]) | (lengths[receiver] == 0), 0, jnp.maximum(slack, 0))
    moved = jax.random.randint(jax.random.fold_in(own, 4), (amount // 2,), 0, 1 << 20) % (slack + 1)
    lengths = lengths.at[giver].add(-moved).at[receiver].add(moved)
    labels = jnp.searchsorted(jnp.cumsum(lengths), jnp.arange(rows * top), side="right").astype(jnp.int32)
    table = labels.reshape(top, rows).T
    table = table[jax.random.permutation(jax.random.fold_in(own, 1), rows)]
    offset_by = jax.random.randint(jax.random.fold_in(own, 2), (rows, 1), 0, top)
    return jnp.take_along_axis(table, (jnp.arange(top)[None, :] + offset_by) % top, axis=1)


def portions_of(amount, total, reach, lean, full):
    loads = [(1 << 20) // math.isqrt(standing ** lean) + 1 for standing in range(1, amount + 1)]
    largest = reach if full else min(reach, max(-(-total // amount), total * loads[0] // sum(loads)))
    least = 1 if total - largest >= amount - 1 else 0
    counts, spare = [largest] + [least] * (amount - 1), total - largest - least * (amount - 1)
    while spare > 0:
        movable = [i for i in range(1, amount) if counts[i] < largest] or [i for i in range(1, amount) if counts[i] < reach]
        pool, left = sum([loads[i] for i in movable]), spare
        for i in movable:
            more = min(reach - counts[i], max(1, left * loads[i] // pool), spare)
            counts[i] = counts[i] + more
            spare = spare - more
    return np.array(counts)


def gaussian(rng, dims, spread, most, cuts=(), kind=jnp.bfloat16):
    result = spread * jax.random.normal(rng, dims, jnp.float32)
    if cuts:
        result = result * block_levels(rng, dims, cuts, -0.22, 0.18)
    return jnp.clip(result, -most, most).astype(kind)


def setup_inputs(seed: int = 0, part: int = 0) -> dict:
    splits = jax.random.split(jax.random.key(seed), 10)
    part_splits = jax.random.split(jax.random.fold_in(splits[9], part), 10)
    slot_pixels = gaussian(part_splits[0], (SLOT_TOTAL, BAND_COUNT, ROWS_DEV, TILE_COLS), 1.0, 6.0, ((0, 8), (1, 2)))
    slot_tile_keys = jax.random.split(jax.random.fold_in(part_splits[1], 1), SLOT_TOTAL // SLOT_DEV)
    slot_tile_turns = jax.random.permutation(jax.random.fold_in(part_splits[1], 3), SLOT_TOTAL // SLOT_DEV)
    slot_tile = jax.vmap(lambda own, number: shared_out(jax.random.fold_in(part_splits[1], 2), own, number, SLOT_DEV, N_SKY, 1, CAPACITY, 2))(slot_tile_keys, slot_tile_turns).reshape((SLOT_TOTAL, 1))
    slot_offset = plant(jax.random.randint(part_splits[2], (SLOT_TOTAL, 2), 0 - MAX_SHIFT, MAX_SHIFT + 1), jax.random.fold_in(part_splits[2], 1), 0 - MAX_SHIFT, MAX_SHIFT).astype(jnp.int32)
    slot_frac = jnp.clip(0.049804688 + 0.89941406 * jax.random.uniform(part_splits[3], (SLOT_TOTAL, 2), jnp.float32) ** block_levels(part_splits[3], (SLOT_TOTAL, 2), ((0, 8),), -0.2, 0.2), 0.049804688, 0.94921875).astype(jnp.bfloat16)
    slot_sigma = jnp.clip(jnp.exp(math.log(2.0) - 1.3862944 * jax.random.uniform(part_splits[4], (SLOT_TOTAL, BAND_COUNT), jnp.float32) ** block_levels(part_splits[4], (SLOT_TOTAL, BAND_COUNT), ((0, 8), (1, 2)), -0.2, 0.2)), 0.5, 2.0).astype(jnp.bfloat16)
    clip_mask = plant((jax.random.randint(part_splits[5], (SLOT_TOTAL, (ROWS_DEV + 2 * MARGIN) // 8, TILE_COLS // 32), 0, 8) < 7).astype(jnp.int32), jax.random.fold_in(part_splits[5], 1), 0, 1)
    slot_count = plant(jax.random.randint(part_splits[6], (N_SKY * N_EPOCH,), 3 * SLOT_DEV // 4, SLOT_DEV + 1), jax.random.fold_in(part_splits[6], 1), 3 * SLOT_DEV // 4, SLOT_DEV).astype(jnp.int32)
    template = gaussian(part_splits[7], (BAND_COUNT, PATCH_ROWS, TILE_COLS), 1.0, 6.0, ((0, 2), (1, 4)))
    prior_weight = jnp.clip(jnp.exp(math.log(4.0) - 2.0794415 * jax.random.uniform(part_splits[8], (BAND_COUNT, PATCH_ROWS), jnp.float32) ** block_levels(part_splits[8], (BAND_COUNT, PATCH_ROWS), ((0, 2), (1, 4)), -0.2, 0.2)), 0.5, 4.0)
    return {"slot_pixels": slot_pixels, "slot_tile": slot_tile, "slot_offset": slot_offset, "slot_frac": slot_frac, "slot_sigma": slot_sigma, "clip_mask": clip_mask, "slot_count": slot_count, "template": template, "prior_weight": prior_weight}


CLIP_WIDTH = 3.0


def lanczos(distance):
    inside = jnp.abs(distance) < 3.0
    return jnp.where(inside, jnp.sinc(distance) * jnp.sinc(distance / 3.0), 0.0)


def tap_weights(fraction):
    steps_back = jnp.arange(-3, 3, dtype=jnp.int32)
    distance = (-steps_back).astype(jnp.float32) - fraction
    rounded = lanczos(distance).astype(jnp.bfloat16)
    return lax.optimization_barrier(rounded).astype(jnp.float32)


def reference(slot_pixels, slot_tile, slot_offset, slot_frac, slot_sigma, clip_mask, slot_count, template, prior_weight):
    slot_number = slot_pixels.shape[0]
    canvas_rows = ROWS_DEV + 2 * MARGIN
    patch_rows = template.shape[1]
    tile_cols = template.shape[2]
    template_pad = jnp.pad(template.astype(jnp.float32), ((0, 0), (MARGIN, MARGIN), (0, 0)))
    empty_sums = jnp.zeros((BAND_COUNT, patch_rows + 2 * MARGIN, tile_cols), jnp.float32)
    row_index = jnp.arange(canvas_rows, dtype=jnp.int32)
    col_index = jnp.arange(tile_cols, dtype=jnp.int32)

    def one_slot(carried, slot_index):
        flux_sums, weight_sums = carried
        pixels = lax.dynamic_index_in_dim(slot_pixels, slot_index, 0, keepdims=False).astype(jnp.float32)
        tile_index = slot_tile[slot_index, 0]
        shift_y = slot_offset[slot_index, 0]
        shift_x = slot_offset[slot_index, 1]
        taps_y = tap_weights(slot_frac[slot_index, 0].astype(jnp.float32))
        taps_x = tap_weights(slot_frac[slot_index, 1].astype(jnp.float32))
        is_live = ((slot_index % SLOT_DEV) < slot_count[slot_index // SLOT_DEV]).astype(jnp.float32)
        padded = jnp.pad(pixels, ((0, 0), (0, 0), (MARGIN, MARGIN)))
        columns = jnp.zeros((BAND_COUNT, ROWS_DEV, tile_cols), jnp.float32)
        col_cover = jnp.zeros((tile_cols,), jnp.float32)
        for tap_index in range(6):
            step_back = tap_index - 3
            shifted = lax.dynamic_slice_in_dim(padded, MARGIN - shift_x + step_back, tile_cols, 2)
            columns = columns + taps_x[tap_index] * shifted
            source_col = col_index - shift_x + step_back
            inside = (source_col >= 0) & (source_col < tile_cols)
            col_cover = col_cover + jnp.where(inside, taps_x[tap_index], 0.0)
        columns = lax.optimization_barrier(columns.astype(jnp.bfloat16)).astype(jnp.float32)
        column_pad = jnp.pad(columns, ((0, 0), (2 * MARGIN, 2 * MARGIN), (0, 0)))
        warped = jnp.zeros((BAND_COUNT, canvas_rows, tile_cols), jnp.float32)
        row_cover = jnp.zeros((canvas_rows,), jnp.float32)
        for tap_index in range(6):
            step_back = tap_index - 3
            shifted = lax.dynamic_slice_in_dim(column_pad, MARGIN - shift_y + step_back, canvas_rows, 1)
            warped = warped + taps_y[tap_index] * shifted
            source_row = row_index - MARGIN - shift_y + step_back
            inside = (source_row >= 0) & (source_row < ROWS_DEV)
            row_cover = row_cover + jnp.where(inside, taps_y[tap_index], 0.0)
        row_cover = jnp.clip(row_cover, 0.0, 1.0)
        col_cover = jnp.clip(col_cover, 0.0, 1.0)
        block_mask = clip_mask[slot_index].astype(jnp.float32)
        expanded = jnp.repeat(jnp.repeat(block_mask, 8, axis=0), 32, axis=1) * is_live
        plane = (expanded * row_cover[:, None]) * col_cover[None, :]
        sigmas = slot_sigma[slot_index].astype(jnp.float32)
        weight = plane[None] / (sigmas * sigmas)[:, None, None]
        framed = lax.dynamic_slice_in_dim(template_pad, tile_index * ROWS_DEV, canvas_rows, 1)
        scale = CLIP_WIDTH * sigmas[:, None, None]
        clipped = framed + scale * jnp.tanh((warped - framed) / scale)
        start = tile_index * ROWS_DEV
        old_flux = lax.dynamic_slice_in_dim(flux_sums, start, canvas_rows, 1)
        old_weight = lax.dynamic_slice_in_dim(weight_sums, start, canvas_rows, 1)
        flux_sums = lax.dynamic_update_slice_in_dim(flux_sums, old_flux + weight * clipped, start, 1)
        weight_sums = lax.dynamic_update_slice_in_dim(weight_sums, old_weight + weight, start, 1)
        return (flux_sums, weight_sums), None

    (flux_sums, weight_sums), _ = lax.scan(one_slot, (empty_sums, empty_sums), jnp.arange(slot_number, dtype=jnp.int32))
    flux_sum = flux_sums[:, MARGIN:MARGIN + patch_rows]
    weight_sum = weight_sums[:, MARGIN:MARGIN + patch_rows]
    prior = prior_weight[:, :, None]
    coadd_image = ((flux_sum + prior * template.astype(jnp.float32)) / (weight_sum + prior)).astype(jnp.bfloat16)
    depth_map = weight_sum + prior
    band_mean = jnp.sum(depth_map, axis=(1, 2)) / (patch_rows * tile_cols)
    depth_norm = (depth_map / band_mean[:, None, None]).astype(jnp.bfloat16)
    return coadd_image, depth_norm
```

```python
import functools

import jax
import jax.numpy as jnp
from jax import lax
from jax.experimental import pallas as pl
from jax.experimental.pallas import tpu as pltpu
from jax.sharding import PartitionSpec as P

MARGIN = 8
BLOCK_ROWS = 8
REACH = 3
LANES = 128
CLIP_WIDTH = 3.0
MESH = pl.DeviceIdType.MESH


def lanczos(distance):
    inside = jnp.abs(distance) < 3.0
    return jnp.where(inside, jnp.sinc(distance) * jnp.sinc(distance / 3.0), 0.0)


def tap_weights(fractions):
    steps_back = jnp.arange(-REACH, REACH, dtype=jnp.int32)
    distance = (-steps_back).astype(jnp.float32) - fractions.astype(jnp.float32)[..., None]
    rounded = lanczos(distance).astype(jnp.bfloat16)
    return lax.optimization_barrier(rounded).astype(jnp.float32)


def gather_kernel(sky, own_ref, all_ref, held, send_sem, recv_sem):
    me = lax.axis_index("sky")
    barrier = pltpu.get_barrier_semaphore()
    for d in range(1, sky):
        pl.semaphore_signal(
            barrier, inc=1, device_id={"sky": lax.rem(me + d, sky)}, device_id_type=MESH
        )
    pl.semaphore_wait(barrier, sky - 1)
    copies = []
    for d in range(1, sky):
        copy = pltpu.make_async_remote_copy(
            src_ref=own_ref,
            dst_ref=held.at[d - 1],
            send_sem=send_sem.at[d - 1],
            recv_sem=recv_sem.at[d - 1],
            device_id={"sky": lax.rem(me + d, sky)},
            device_id_type=MESH,
        )
        copy.start()
        copies.append(copy)
    all_ref[me] = own_ref[...]
    for d in range(1, sky):
        copies[d - 1].wait()
        all_ref[lax.rem(me - d + sky, sky)] = held[d - 1]


def warp_kernel(
    bands, sky, epochs, rows,
    tile_ref, offset_ref, taps_ref, sigma_ref,
    pixels_ref, mask_ref, template_ref, prior_ref,
    send_ref, total_ref,
    framed, flux, weights, source, wide_mask,
):
    slots = pixels_ref.shape[0]
    cols = pixels_ref.shape[2]
    padded = cols + LANES
    canvas = rows + 2 * MARGIN
    blocks = canvas // BLOCK_ROWS
    part = cols // epochs
    mask_cols = mask_ref.shape[1]

    flux[...] = jnp.zeros_like(flux)
    weights[...] = jnp.zeros_like(weights)
    edge = jnp.zeros((bands, MARGIN, cols), jnp.float32)
    framed[:, :MARGIN] = edge
    framed[:, MARGIN + sky * rows :] = edge
    for s in range(sky):
        framed[:, MARGIN + s * rows : MARGIN + (s + 1) * rows] = template_ref[s].astype(jnp.float32)
    source[:, cols:] = jnp.zeros((source.shape[0], LANES), jnp.float32)
    source[bands * rows :, :cols] = jnp.ones((8, cols), jnp.float32)
    cell = lax.broadcasted_iota(jnp.int32, (mask_cols, cols), 0)
    column = lax.broadcasted_iota(jnp.int32, (mask_cols, cols), 1) // (cols // mask_cols)
    spread = jnp.where(cell == column, 1.0, 0.0).astype(jnp.bfloat16)
    wide_mask[...] = jnp.dot(
        mask_ref[...], spread, preferred_element_type=jnp.float32
    ).reshape(wide_mask.shape)
    gap = (
        lax.broadcasted_iota(jnp.int32, (canvas, rows), 0)
        - lax.broadcasted_iota(jnp.int32, (canvas, rows), 1)
        - MARGIN
    )

    def one_slot(p, carry):
        dy, dx = offset_ref[p, 0], offset_ref[p, 1]
        source[: bands * rows, :cols] = pixels_ref[p].astype(jnp.float32)
        base = pltpu.roll(source[...], lax.rem(dx + padded, padded), 1)
        summed = taps_ref[p, 2 * REACH + REACH] * base
        for tap in range(2 * REACH):
            if tap != REACH:
                moved = pltpu.roll(base, (REACH - tap) % padded, 1)
                summed = summed + taps_ref[p, 2 * REACH + tap] * moved
        columns = summed[: bands * rows, :cols].astype(jnp.bfloat16)
        col_cover = jnp.clip(summed[bands * rows :, :cols], 0.0, 1.0)
        row_table = jnp.zeros((canvas, rows), jnp.float32)
        for tap in range(2 * REACH):
            row_table = row_table + jnp.where(gap == dy + REACH - tap, taps_ref[p, tap], 0.0)
        row_cover = jnp.clip(jnp.sum(row_table, 1, keepdims=True), 0.0, 1.0)
        row_table = row_table.astype(jnp.bfloat16)
        pieces = []
        for i in range(blocks):
            cover = row_cover[i * BLOCK_ROWS : (i + 1) * BLOCK_ROWS]
            pieces.append(wide_mask[p, i : i + 1] * cover * col_cover)
        plane = jnp.concatenate(pieces, 0)
        start = pl.multiple_of(tile_ref[p] * rows, 8)
        for b in range(bands):
            warped = jnp.dot(
                row_table, columns[b * rows : (b + 1) * rows], preferred_element_type=jnp.float32
            )
            frame = framed[b, pl.ds(start, canvas)]
            scale = sigma_ref[p, b]
            clipped = frame + scale * jnp.tanh((warped - frame) * sigma_ref[p, bands + b])
            weight = plane * sigma_ref[p, 2 * bands + b]
            flux[b, pl.ds(start, canvas)] += weight * clipped
            weights[b, pl.ds(start, canvas)] += weight
        return carry

    lax.fori_loop(0, slots, one_slot, 0)
    for s in range(sky):
        near = slice(MARGIN + s * rows, MARGIN + (s + 1) * rows)
        for e in range(epochs):
            far = slice(e * part, (e + 1) * part)
            send_ref[s * epochs + e, 0] = flux[:, near, far].astype(jnp.bfloat16)
            send_ref[s * epochs + e, 1] = weights[:, near, far].astype(jnp.bfloat16)
    total_ref[...] = jnp.zeros_like(total_ref)
    for b in range(bands):
        along = jnp.sum(weights[b, MARGIN : MARGIN + sky * rows], 0, keepdims=True)
        folded = along[:, :LANES]
        for c in range(1, cols // LANES):
            folded = folded + along[:, c * LANES : (c + 1) * LANES]
        prior = jnp.sum(prior_ref[b], 0, keepdims=True)
        total_ref[b : b + 1] = folded + prior * (part / LANES)


def exchange_kernel(
    bands, sky, epochs, pixels_all,
    send_ref, total_ref, template_ref, prior_ref,
    coadd_ref, depth_ref,
    held, held_total, send_sem, recv_sem, send_total_sem, recv_total_sem,
):
    count = sky * epochs
    part = coadd_ref.shape[2]
    epoch = lax.axis_index("epoch")
    me = lax.axis_index("sky") * epochs + epoch

    def peer(d):
        index = lax.rem(me + d, count)
        return index, {"sky": index // epochs, "epoch": lax.rem(index, epochs)}

    barrier = pltpu.get_barrier_semaphore()
    for d in range(1, count):
        pl.semaphore_signal(barrier, inc=1, device_id=peer(d)[1], device_id_type=MESH)
    pl.semaphore_wait(barrier, count - 1)
    copies = []
    for d in range(1, count):
        index, where = peer(d)
        small = pltpu.make_async_remote_copy(
            src_ref=total_ref,
            dst_ref=held_total.at[d - 1],
            send_sem=send_total_sem.at[d - 1],
            recv_sem=recv_total_sem.at[d - 1],
            device_id=where,
            device_id_type=MESH,
        )
        small.start()
        large = pltpu.make_async_remote_copy(
            src_ref=send_ref.at[index],
            dst_ref=held.at[d - 1],
            send_sem=send_sem.at[d - 1],
            recv_sem=recv_sem.at[d - 1],
            device_id=where,
            device_id_type=MESH,
        )
        large.start()
        copies.append((small, large))
    for small, large in copies:
        small.wait()
        large.wait()
    total = total_ref[...]
    for d in range(1, count):
        total = total + held_total[d - 1]
    mean = jnp.sum(total, 1, keepdims=True) * (1.0 / pixels_all)
    for b in range(bands):
        flux = send_ref[me, 0, b].astype(jnp.float32)
        weight = send_ref[me, 1, b].astype(jnp.float32)
        for d in range(1, count):
            flux = flux + held[d - 1, 0, b].astype(jnp.float32)
            weight = weight + held[d - 1, 1, b].astype(jnp.float32)
        prior = prior_ref[b]
        columns = pl.ds(pl.multiple_of(epoch * part, LANES), part)
        template = template_ref[b, :, columns].astype(jnp.float32)
        depth = weight + prior
        coadd_ref[b] = ((flux + prior * template) / depth).astype(jnp.bfloat16)
        depth_ref[b] = (depth / mean[b : b + 1]).astype(jnp.bfloat16)


def on_device(
    slot_pixels, slot_tile, slot_offset, slot_frac, slot_sigma, clip_mask, slot_count, template, prior_weight
):
    sky = lax.axis_size("sky")
    epochs = lax.axis_size("epoch")
    count = sky * epochs
    slots, bands, rows, cols = slot_pixels.shape
    canvas = rows + 2 * MARGIN
    part = cols // epochs
    vmem = pl.BlockSpec(memory_space=pltpu.VMEM)
    smem = pl.BlockSpec(memory_space=pltpu.SMEM)
    templates = pl.pallas_call(
        functools.partial(gather_kernel, sky),
        out_shape=jax.ShapeDtypeStruct((sky,) + template.shape, jnp.bfloat16),
        in_specs=[vmem],
        out_specs=vmem,
        scratch_shapes=[
            pltpu.VMEM((sky - 1,) + template.shape, jnp.bfloat16),
            pltpu.SemaphoreType.DMA((sky - 1,)),
            pltpu.SemaphoreType.DMA((sky - 1,)),
        ],
        compiler_params=pltpu.CompilerParams(collective_id=0, has_side_effects=True),
        name="gather_templates",
    )(template)
    is_live = (jnp.arange(slots, dtype=jnp.int32) < slot_count[0]).astype(jnp.int32)
    mask_rows = clip_mask.shape[1]
    mask = (clip_mask * is_live[:, None, None]).astype(jnp.bfloat16)
    mask = jnp.pad(mask, ((0, 0), (0, -mask_rows % 8), (0, 0)))
    mask_rows = mask.shape[1]
    mask = mask.reshape(slots * mask_rows, mask.shape[2])
    taps = tap_weights(slot_frac).reshape(slots, 4 * REACH)
    sigma = slot_sigma.astype(jnp.float32)
    scale = CLIP_WIDTH * sigma
    sigmas = jnp.concatenate([scale, 1.0 / scale, 1.0 / (sigma * sigma)], 1)
    prior = prior_weight[:, :, None]
    patch = sky * rows + 2 * MARGIN
    sums = pltpu.VMEM((bands, patch, cols), jnp.float32)
    send, total = pl.pallas_call(
        functools.partial(warp_kernel, bands, sky, epochs, rows),
        out_shape=(
            jax.ShapeDtypeStruct((count, 2, bands, rows, part), jnp.bfloat16),
            jax.ShapeDtypeStruct((8 * -(-bands // 8), LANES), jnp.float32),
        ),
        in_specs=[smem] * 4 + [vmem] * 4,
        out_specs=(vmem, vmem),
        scratch_shapes=[
            sums,
            sums,
            sums,
            pltpu.VMEM((bands * rows + 8, cols + LANES), jnp.float32),
            pltpu.VMEM((slots, mask_rows, cols), jnp.float32),
        ],
        name="warp_slots",
    )(
        slot_tile[:, 0], slot_offset, taps, sigmas,
        slot_pixels.reshape(slots, bands * rows, cols), mask, templates, prior,
    )
    block = jax.ShapeDtypeStruct((bands, rows, part), jnp.bfloat16)
    return pl.pallas_call(
        functools.partial(exchange_kernel, bands, sky, epochs, sky * rows * cols),
        out_shape=(block, block),
        in_specs=[vmem] * 4,
        out_specs=(vmem, vmem),
        scratch_shapes=[
            pltpu.VMEM((count - 1,) + send.shape[1:], jnp.bfloat16),
            pltpu.VMEM((count - 1,) + total.shape, jnp.float32),
            pltpu.SemaphoreType.DMA((count - 1,)),
            pltpu.SemaphoreType.DMA((count - 1,)),
            pltpu.SemaphoreType.DMA((count - 1,)),
            pltpu.SemaphoreType.DMA((count - 1,)),
        ],
        compiler_params=pltpu.CompilerParams(collective_id=1, has_side_effects=True),
        name="exchange_sums",
    )(send, total, template, prior)


def solution(mesh):
    in_specs = (
        P(("groups", "sky", "epoch"), "band", None, None),
        P(("groups", "sky", "epoch"), None),
        P(("groups", "sky", "epoch"), None),
        P(("groups", "sky", "epoch"), None),
        P(("groups", "sky", "epoch"), "band"),
        P(("groups", "sky", "epoch"), None, None),
        P(("groups", "sky", "epoch")),
        P("band", ("groups", "sky"), None),
        P("band", ("groups", "sky")),
    )
    out_specs = (P("band", ("groups", "sky"), "epoch"), P("band", ("groups", "sky"), "epoch"))
    return jax.shard_map(
        on_device, mesh=mesh, in_specs=in_specs, out_specs=out_specs, check_vma=False
    )
```

```python
import functools

import jax
import jax.numpy as jnp
from jax import lax
from jax.experimental import pallas as pl
from jax.experimental.pallas import tpu as pltpu
from jax.sharding import PartitionSpec as P

MARGIN = 8
BLOCK_ROWS = 8
REACH = 3
LANES = 128
CLIP_WIDTH = 3.0
CELL_TYPE = jnp.bfloat16
MESH = pl.DeviceIdType.MESH


def lanczos(distance):
    inside = jnp.abs(distance) < 3.0
    return jnp.where(inside, jnp.sinc(distance) * jnp.sinc(distance / 3.0), 0.0)


def tap_weights(fractions):
    steps_back = jnp.arange(-REACH, REACH, dtype=jnp.int32)
    distance = (-steps_back).astype(jnp.float32) - fractions.astype(jnp.float32)[..., None]
    rounded = lanczos(distance).astype(jnp.bfloat16)
    return lax.optimization_barrier(rounded).astype(jnp.float32)


def gather_kernel(sky, own_ref, all_ref, held, send_sem, recv_sem):
    me = lax.axis_index("sky")
    barrier = pltpu.get_barrier_semaphore()
    for d in range(1, sky):
        pl.semaphore_signal(
            barrier, inc=1, device_id={"sky": lax.rem(me + d, sky)}, device_id_type=MESH
        )
    pl.semaphore_wait(barrier, sky - 1)
    copies = []
    for d in range(1, sky):
        copy = pltpu.make_async_remote_copy(
            src_ref=own_ref,
            dst_ref=held.at[d - 1],
            send_sem=send_sem.at[d - 1],
            recv_sem=recv_sem.at[d - 1],
            device_id={"sky": lax.rem(me + d, sky)},
            device_id_type=MESH,
        )
        copy.start()
        copies.append(copy)
    all_ref[me] = own_ref[...]
    for d in range(1, sky):
        copies[d - 1].wait()
        all_ref[lax.rem(me - d + sky, sky)] = held[d - 1]


def warp_kernel(
    bands, sky, epochs, rows,
    tile_ref, offset_ref, taps_ref, sigma_ref,
    pixels_ref, mask_ref, template_ref, prior_ref,
    send_ref, total_ref, rows_ref, cells_ref,
    framed, flux, cells, source, wide_mask,
):
    slots = pixels_ref.shape[0]
    cols = pixels_ref.shape[2]
    padded = cols + LANES
    canvas = rows + 2 * MARGIN
    blocks = canvas // BLOCK_ROWS
    part = cols // epochs
    mask_cols = mask_ref.shape[1]

    flux[...] = jnp.zeros_like(flux)
    cells[...] = jnp.zeros_like(cells)
    total_ref[...] = jnp.zeros_like(total_ref)
    rows_ref[...] = jnp.zeros_like(rows_ref)
    lane = lax.broadcasted_iota(jnp.int32, (sky, rows_ref.shape[2]), 1)
    patch_row = lax.broadcasted_iota(jnp.int32, lane.shape, 0) * rows + lax.rem(lane, rows)
    canvas_row = lax.broadcasted_iota(jnp.int32, (canvas, 1), 0) - MARGIN
    group = rows // BLOCK_ROWS
    first = MARGIN // BLOCK_ROWS
    edge = jnp.zeros((bands, MARGIN, cols), jnp.float32)
    framed[:, :MARGIN] = edge
    framed[:, MARGIN + sky * rows :] = edge
    for s in range(sky):
        framed[:, MARGIN + s * rows : MARGIN + (s + 1) * rows] = template_ref[s].astype(jnp.float32)
    source[:, cols:] = jnp.zeros((source.shape[0], LANES), jnp.float32)
    source[bands * rows :, :cols] = jnp.ones((8, cols), jnp.float32)
    cell = lax.broadcasted_iota(jnp.int32, (mask_cols, cols), 0)
    column = lax.broadcasted_iota(jnp.int32, (mask_cols, cols), 1) // (cols // mask_cols)
    spread = jnp.where(cell == column, 1.0, 0.0).astype(jnp.bfloat16)
    wide_mask[...] = jnp.dot(
        mask_ref[...], spread, preferred_element_type=jnp.float32
    ).reshape(wide_mask.shape)
    gap = (
        lax.broadcasted_iota(jnp.int32, (canvas, rows), 0)
        - lax.broadcasted_iota(jnp.int32, (canvas, rows), 1)
        - MARGIN
    )

    def one_slot(p, carry):
        dy, dx = offset_ref[p, 0], offset_ref[p, 1]
        source[: bands * rows, :cols] = pixels_ref[p].astype(jnp.float32)
        base = pltpu.roll(source[...], lax.rem(dx + padded, padded), 1)
        summed = taps_ref[p, 2 * REACH + REACH] * base
        for tap in range(2 * REACH):
            if tap != REACH:
                moved = pltpu.roll(base, (REACH - tap) % padded, 1)
                summed = summed + taps_ref[p, 2 * REACH + tap] * moved
        columns = summed[: bands * rows, :cols].astype(jnp.bfloat16)
        col_cover = jnp.clip(summed[bands * rows :, :cols], 0.0, 1.0)
        row_table = jnp.zeros((canvas, rows), jnp.float32)
        for tap in range(2 * REACH):
            row_table = row_table + jnp.where(gap == dy + REACH - tap, taps_ref[p, tap], 0.0)
        row_cover = jnp.clip(jnp.sum(row_table, 1, keepdims=True), 0.0, 1.0)
        row_table = row_table.astype(jnp.bfloat16)
        start = pl.multiple_of(tile_ref[p] * rows, 8)
        global_row = canvas_row + start
        row_cover = jnp.where((global_row >= 0) & (global_row < sky * rows), row_cover, 0.0)
        pieces = []
        for i in range(blocks):
            cover = row_cover[i * BLOCK_ROWS : (i + 1) * BLOCK_ROWS]
            cell_row = wide_mask[p, i : i + 1] * col_cover[:1]
            cells[tile_ref[p] * group + i, pl.ds(p, 1)] = cell_row
            pieces.append(cell_row * cover)
        plane = jnp.concatenate(pieces, 0)
        tile_row = patch_row - start - dy
        profile = jnp.zeros(lane.shape, jnp.float32)
        for tap in range(2 * REACH):
            from_row = tile_row + (tap - REACH)
            profile = profile + jnp.where((from_row >= 0) & (from_row < rows), taps_ref[p, tap], 0.0)
        profile = jnp.clip(profile, 0.0, 1.0)
        inverse = jnp.zeros(lane.shape, jnp.float32)
        along = jnp.sum(plane, 0, keepdims=True)
        folded = along[:, :LANES]
        for c in range(1, cols // LANES):
            folded = folded + along[:, c * LANES : (c + 1) * LANES]
        for b in range(bands):
            inverse = jnp.where(lane // rows == b, sigma_ref[p, 2 * bands + b], inverse)
            total_ref[b : b + 1] += folded * sigma_ref[p, 2 * bands + b]
        profile = profile * inverse
        for s in range(sky):
            rows_ref[s, pl.ds(p, 1)] = profile[s : s + 1]
        for b in range(bands):
            warped = jnp.dot(
                row_table, columns[b * rows : (b + 1) * rows], preferred_element_type=jnp.float32
            )
            frame = framed[b, pl.ds(start, canvas)]
            scale = sigma_ref[p, b]
            clipped = frame + scale * jnp.tanh((warped - frame) * sigma_ref[p, bands + b])
            weight = plane * sigma_ref[p, 2 * bands + b]
            flux[b, pl.ds(start, canvas)] += weight * clipped
        return carry

    lax.fori_loop(0, slots, one_slot, 0)
    for s in range(sky):
        near = slice(MARGIN + s * rows, MARGIN + (s + 1) * rows)
        for e in range(epochs):
            far = slice(e * part, (e + 1) * part)
            send_ref[s * epochs + e] = flux[:, near, far].astype(jnp.bfloat16)
            for g in range(group):
                cells_ref[s * epochs + e, g] = cells[first + s * group + g, :, far].astype(CELL_TYPE)
    for b in range(bands):
        prior = jnp.sum(prior_ref[b], 0, keepdims=True)
        total_ref[b : b + 1] += prior * (part / LANES)


def exchange_kernel(
    bands, sky, epochs, pixels_all,
    send_ref, total_ref, rows_ref, cells_ref, template_ref, prior_ref,
    coadd_ref, depth_ref,
    held, held_total, held_rows, held_cells, send_sem, recv_sem,
):
    count = sky * epochs
    part = coadd_ref.shape[2]
    epoch = lax.axis_index("epoch")
    me = lax.axis_index("sky") * epochs + epoch

    def peer(d):
        index = lax.rem(me + d, count)
        return index, {"sky": index // epochs, "epoch": lax.rem(index, epochs)}

    barrier = pltpu.get_barrier_semaphore()
    for d in range(1, count):
        pl.semaphore_signal(barrier, inc=1, device_id=peer(d)[1], device_id_type=MESH)
    pl.semaphore_wait(barrier, count - 1)
    copies = []
    for d in range(1, count):
        index, where = peer(d)
        sky_index = index // epochs
        moves = (
            (total_ref, held_total),
            (rows_ref.at[sky_index], held_rows),
            (cells_ref.at[index], held_cells),
            (send_ref.at[index], held),
        )
        for k, (src, dst) in enumerate(moves):
            copy = pltpu.make_async_remote_copy(
                src_ref=src,
                dst_ref=dst.at[d - 1],
                send_sem=send_sem.at[k, d - 1],
                recv_sem=recv_sem.at[k, d - 1],
                device_id=where,
                device_id_type=MESH,
            )
            copy.start()
            copies.append(copy)
    for copy in copies:
        copy.wait()
    total = total_ref[...]
    for d in range(1, count):
        total = total + held_total[d - 1]
    mean = jnp.sum(total, 1, keepdims=True) * (1.0 / pixels_all)
    rows = template_ref.shape[1]
    group = rows // BLOCK_ROWS
    sky_me = lax.axis_index("sky")

    def weight_from(profile, cell):
        block = lax.broadcasted_iota(jnp.int32, profile.shape, 1) // BLOCK_ROWS
        block = lax.rem(block, group)
        wide = [jnp.where(block == g, profile, 0.0) for g in range(group)]
        wide = jnp.concatenate(wide, 0).astype(jnp.bfloat16)
        cell = jnp.concatenate([cell[g].astype(jnp.float32) for g in range(group)], 0)
        return lax.dot_general(
            wide, cell.astype(jnp.bfloat16), (((0,), (0,)), ((), ())),
            preferred_element_type=jnp.float32,
        )

    weights = weight_from(rows_ref[sky_me], cells_ref[me])
    for d in range(1, count):
        weights = weights + weight_from(held_rows[d - 1], held_cells[d - 1])
    for b in range(bands):
        flux = send_ref[me, b].astype(jnp.float32)
        weight = weights[b * rows : (b + 1) * rows]
        for d in range(1, count):
            flux = flux + held[d - 1, b].astype(jnp.float32)
        prior = prior_ref[b]
        columns = pl.ds(pl.multiple_of(epoch * part, LANES), part)
        template = template_ref[b, :, columns].astype(jnp.float32)
        depth = weight + prior
        coadd_ref[b] = ((flux + prior * template) / depth).astype(jnp.bfloat16)
        depth_ref[b] = (depth / mean[b : b + 1]).astype(jnp.bfloat16)


def on_device(
    slot_pixels, slot_tile, slot_offset, slot_frac, slot_sigma, clip_mask, slot_count, template, prior_weight
):
    sky = lax.axis_size("sky")
    epochs = lax.axis_size("epoch")
    count = sky * epochs
    slots, bands, rows, cols = slot_pixels.shape
    canvas = rows + 2 * MARGIN
    part = cols // epochs
    vmem = pl.BlockSpec(memory_space=pltpu.VMEM)
    smem = pl.BlockSpec(memory_space=pltpu.SMEM)
    templates = pl.pallas_call(
        functools.partial(gather_kernel, sky),
        out_shape=jax.ShapeDtypeStruct((sky,) + template.shape, jnp.bfloat16),
        in_specs=[vmem],
        out_specs=vmem,
        scratch_shapes=[
            pltpu.VMEM((sky - 1,) + template.shape, jnp.bfloat16),
            pltpu.SemaphoreType.DMA((sky - 1,)),
            pltpu.SemaphoreType.DMA((sky - 1,)),
        ],
        compiler_params=pltpu.CompilerParams(collective_id=0, has_side_effects=True),
        name="gather_templates",
    )(template)
    is_live = (jnp.arange(slots, dtype=jnp.int32) < slot_count[0]).astype(jnp.int32)
    mask_rows = clip_mask.shape[1]
    mask = (clip_mask * is_live[:, None, None]).astype(jnp.bfloat16)
    mask = jnp.pad(mask, ((0, 0), (0, -mask_rows % 8), (0, 0)))
    mask_rows = mask.shape[1]
    mask = mask.reshape(slots * mask_rows, mask.shape[2])
    taps = tap_weights(slot_frac).reshape(slots, 4 * REACH)
    sigma = slot_sigma.astype(jnp.float32)
    scale = CLIP_WIDTH * sigma
    sigmas = jnp.concatenate([scale, 1.0 / scale, 1.0 / (sigma * sigma)], 1)
    prior = prior_weight[:, :, None]
    patch = sky * rows + 2 * MARGIN
    sums = pltpu.VMEM((bands, patch, cols), jnp.float32)
    held_slots = slots + -slots % 8
    lanes = bands * rows + -(bands * rows) % LANES
    group = rows // BLOCK_ROWS
    patch_blocks = sky * group + 2 * MARGIN // BLOCK_ROWS
    send, total, row_factor, cell_factor = pl.pallas_call(
        functools.partial(warp_kernel, bands, sky, epochs, rows),
        out_shape=(
            jax.ShapeDtypeStruct((count, bands, rows, part), jnp.bfloat16),
            jax.ShapeDtypeStruct((8 * -(-bands // 8), LANES), jnp.float32),
            jax.ShapeDtypeStruct((sky, held_slots, lanes), jnp.float32),
            jax.ShapeDtypeStruct((count, group, held_slots, part), CELL_TYPE),
        ),
        in_specs=[smem] * 4 + [vmem] * 4,
        out_specs=(vmem,) * 4,
        scratch_shapes=[
            sums,
            sums,
            pltpu.VMEM((patch_blocks, held_slots, cols), jnp.float32),
            pltpu.VMEM((bands * rows + 8, cols + LANES), jnp.float32),
            pltpu.VMEM((slots, mask_rows, cols), jnp.float32),
        ],
        name="warp_slots",
    )(
        slot_tile[:, 0], slot_offset, taps, sigmas,
        slot_pixels.reshape(slots, bands * rows, cols), mask, templates, prior,
    )
    block = jax.ShapeDtypeStruct((bands, rows, part), jnp.bfloat16)
    return pl.pallas_call(
        functools.partial(exchange_kernel, bands, sky, epochs, sky * rows * cols),
        out_shape=(block, block),
        in_specs=[vmem] * 6,
        out_specs=(vmem, vmem),
        scratch_shapes=[
            pltpu.VMEM((count - 1,) + send.shape[1:], jnp.bfloat16),
            pltpu.VMEM((count - 1,) + total.shape, jnp.float32),
            pltpu.VMEM((count - 1,) + row_factor.shape[1:], jnp.float32),
            pltpu.VMEM((count - 1,) + cell_factor.shape[1:], CELL_TYPE),
            pltpu.SemaphoreType.DMA((4, count - 1)),
            pltpu.SemaphoreType.DMA((4, count - 1)),
        ],
        compiler_params=pltpu.CompilerParams(collective_id=1, has_side_effects=True),
        name="exchange_sums",
    )(send, total, row_factor, cell_factor, template, prior)


def solution(mesh):
    in_specs = (
        P(("groups", "sky", "epoch"), "band", None, None),
        P(("groups", "sky", "epoch"), None),
        P(("groups", "sky", "epoch"), None),
        P(("groups", "sky", "epoch"), None),
        P(("groups", "sky", "epoch"), "band"),
        P(("groups", "sky", "epoch"), None, None),
        P(("groups", "sky", "epoch")),
        P("band", ("groups", "sky"), None),
        P("band", ("groups", "sky")),
    )
    out_specs = (P("band", ("groups", "sky"), "epoch"), P("band", ("groups", "sky"), "epoch"))
    return jax.shard_map(
        on_device, mesh=mesh, in_specs=in_specs, out_specs=out_specs, check_vma=False
    )
```

```python
import functools

import jax
import jax.numpy as jnp
from jax import lax
from jax.experimental import pallas as pl
from jax.experimental.pallas import tpu as pltpu
from jax.sharding import PartitionSpec as P

MARGIN = 8
BLOCK_ROWS = 8
REACH = 3
LANES = 128
CLIP_WIDTH = 3.0
CELL_TYPE = jnp.bfloat16
MESH = pl.DeviceIdType.MESH


def lanczos(distance):
    inside = jnp.abs(distance) < 3.0
    return jnp.where(inside, jnp.sinc(distance) * jnp.sinc(distance / 3.0), 0.0)


def tap_weights(fractions):
    steps_back = jnp.arange(-REACH, REACH, dtype=jnp.int32)
    distance = (-steps_back).astype(jnp.float32)[:, None] - fractions.astype(jnp.float32)[:, None]
    rounded = lanczos(distance).astype(jnp.bfloat16)
    return lax.optimization_barrier(rounded).astype(jnp.float32)


def gather_kernel(sky, own_ref, all_ref, held, send_sem, recv_sem):
    me = lax.axis_index("sky")
    barrier = pltpu.get_barrier_semaphore()
    for d in range(1, sky):
        pl.semaphore_signal(
            barrier, inc=1, device_id={"sky": lax.rem(me + d, sky)}, device_id_type=MESH
        )
    pl.semaphore_wait(barrier, sky - 1)
    copies = []
    for d in range(1, sky):
        copy = pltpu.make_async_remote_copy(
            src_ref=own_ref,
            dst_ref=held.at[d - 1],
            send_sem=send_sem.at[d - 1],
            recv_sem=recv_sem.at[d - 1],
            device_id={"sky": lax.rem(me + d, sky)},
            device_id_type=MESH,
        )
        copy.start()
        copies.append(copy)
    all_ref[me] = own_ref[...]
    for d in range(1, sky):
        copies[d - 1].wait()
        all_ref[lax.rem(me - d + sky, sky)] = held[d - 1]


def warp_kernel(
    bands, sky, epochs, rows,
    tile_ref, offset_ref, count_ref, param_ref,
    pixels_ref, mask_ref, template_ref, prior_ref,
    send_ref, total_ref, rows_ref, cells_ref,
    framed, flux, cells, source,
):
    slots = pixels_ref.shape[0]
    cols = pixels_ref.shape[2]
    padded = cols + LANES
    canvas = rows + 2 * MARGIN
    blocks = canvas // BLOCK_ROWS
    part = cols // epochs
    mask_cols = mask_ref.shape[2]

    flux[...] = jnp.zeros_like(flux)
    cells[...] = jnp.zeros_like(cells)
    total_ref[...] = jnp.zeros_like(total_ref)
    rows_ref[...] = jnp.zeros_like(rows_ref)
    lane = lax.broadcasted_iota(jnp.int32, (sky, rows_ref.shape[2]), 1)
    patch_row = lax.broadcasted_iota(jnp.int32, lane.shape, 0) * rows + lax.rem(lane, rows)
    canvas_row = lax.broadcasted_iota(jnp.int32, (canvas, 1), 0) - MARGIN
    group = rows // BLOCK_ROWS
    first = MARGIN // BLOCK_ROWS
    edge = jnp.zeros((bands, MARGIN, cols), jnp.float32)
    framed[:, :MARGIN] = edge
    framed[:, MARGIN + sky * rows :] = edge
    for s in range(sky):
        framed[:, MARGIN + s * rows : MARGIN + (s + 1) * rows] = template_ref[s].astype(jnp.float32)
    source[:, cols:] = jnp.zeros((source.shape[0], LANES), jnp.float32)
    source[bands * rows :, :cols] = jnp.ones((8, cols), jnp.float32)
    cell = lax.broadcasted_iota(jnp.int32, (mask_cols, cols), 0)
    column = lax.broadcasted_iota(jnp.int32, (mask_cols, cols), 1) // (cols // mask_cols)
    spread = jnp.where(cell == column, 1.0, 0.0).astype(jnp.bfloat16)
    gap = (
        lax.broadcasted_iota(jnp.int32, (canvas, rows), 0)
        - lax.broadcasted_iota(jnp.int32, (canvas, rows), 1)
        - MARGIN
    )

    def one_slot(p, carry):
        dy, dx = offset_ref[0, p], offset_ref[1, p]
        source[: bands * rows, :cols] = pixels_ref[p].astype(jnp.float32)
        base = pltpu.roll(source[...], lax.rem(dx + padded, padded), 1)
        summed = param_ref[2 * REACH + REACH, p] * base
        for tap in range(2 * REACH):
            if tap != REACH:
                moved = pltpu.roll(base, (REACH - tap) % padded, 1)
                summed = summed + param_ref[2 * REACH + tap, p] * moved
        columns = summed[: bands * rows, :cols].astype(jnp.bfloat16)
        col_cover = jnp.clip(summed[bands * rows :, :cols], 0.0, 1.0)
        row_table = jnp.zeros((canvas, rows), jnp.float32)
        for tap in range(2 * REACH):
            row_table = row_table + jnp.where(gap == dy + REACH - tap, param_ref[tap, p], 0.0)
        row_cover = jnp.clip(jnp.sum(row_table, 1, keepdims=True), 0.0, 1.0)
        row_table = row_table.astype(jnp.bfloat16)
        start = pl.multiple_of(tile_ref[p] * rows, 8)
        global_row = canvas_row + start
        row_cover = jnp.where((global_row >= 0) & (global_row < sky * rows), row_cover, 0.0)
        live = jnp.where(p < count_ref[0], 1.0, 0.0)
        wide_mask = live * jnp.dot(
            mask_ref[p].astype(jnp.bfloat16), spread, preferred_element_type=jnp.float32
        )
        pieces = []
        for i in range(blocks):
            cover = row_cover[i * BLOCK_ROWS : (i + 1) * BLOCK_ROWS]
            cell_row = wide_mask[i : i + 1] * col_cover[:1]
            cells[tile_ref[p] * group + i, pl.ds(p, 1)] = cell_row
            pieces.append(cell_row * cover)
        plane = jnp.concatenate(pieces, 0)
        tile_row = patch_row - start - dy
        profile = jnp.zeros(lane.shape, jnp.float32)
        for tap in range(2 * REACH):
            from_row = tile_row + (tap - REACH)
            profile = profile + jnp.where((from_row >= 0) & (from_row < rows), param_ref[tap, p], 0.0)
        profile = jnp.clip(profile, 0.0, 1.0)
        inverse = jnp.zeros(lane.shape, jnp.float32)
        along = jnp.sum(plane, 0, keepdims=True)
        folded = along[:, :LANES]
        for c in range(1, cols // LANES):
            folded = folded + along[:, c * LANES : (c + 1) * LANES]
        for b in range(bands):
            inverse = jnp.where(lane // rows == b, param_ref[4 * REACH + 2 * bands + b, p], inverse)
            total_ref[b : b + 1] += folded * param_ref[4 * REACH + 2 * bands + b, p]
        profile = profile * inverse
        for s in range(sky):
            rows_ref[s, pl.ds(p, 1)] = profile[s : s + 1]
        for b in range(bands):
            warped = jnp.dot(
                row_table, columns[b * rows : (b + 1) * rows], preferred_element_type=jnp.float32
            )
            frame = framed[b, pl.ds(start, canvas)]
            scale = param_ref[4 * REACH + b, p]
            clipped = frame + scale * jnp.tanh((warped - frame) * param_ref[4 * REACH + bands + b, p])
            weight = plane * param_ref[4 * REACH + 2 * bands + b, p]
            flux[b, pl.ds(start, canvas)] += weight * clipped
        return carry

    lax.fori_loop(0, slots, one_slot, 0)
    for s in range(sky):
        near = slice(MARGIN + s * rows, MARGIN + (s + 1) * rows)
        for e in range(epochs):
            far = slice(e * part, (e + 1) * part)
            send_ref[s * epochs + e] = flux[:, near, far].astype(jnp.bfloat16)
            for g in range(group):
                cells_ref[s * epochs + e, g] = cells[first + s * group + g, :, far].astype(CELL_TYPE)
    for b in range(bands):
        prior = jnp.sum(prior_ref[b : b + 1], 1, keepdims=True)
        total_ref[b : b + 1] += prior * (part / LANES)


def exchange_kernel(
    bands, sky, epochs, pixels_all,
    send_ref, total_ref, rows_ref, cells_ref, template_ref, prior_ref,
    coadd_ref, depth_ref,
    held, held_total, held_rows, held_cells, send_sem, recv_sem,
):
    count = sky * epochs
    part = coadd_ref.shape[2]
    epoch = lax.axis_index("epoch")
    me = lax.axis_index("sky") * epochs + epoch

    def peer(d):
        index = lax.rem(me + d, count)
        return index, {"sky": index // epochs, "epoch": lax.rem(index, epochs)}

    barrier = pltpu.get_barrier_semaphore()
    for d in range(1, count):
        pl.semaphore_signal(barrier, inc=1, device_id=peer(d)[1], device_id_type=MESH)
    pl.semaphore_wait(barrier, count - 1)
    copies = []
    for large in (False, True):
        for d in range(1, count):
            index, where = peer(d)
            moves = (
                (send_ref.at[index], held),
                (total_ref, held_total),
                (rows_ref.at[index // epochs], held_rows),
                (cells_ref.at[index], held_cells),
            )
            for k, (src, dst) in enumerate(moves):
                if large == (k == 0):
                    copy = pltpu.make_async_remote_copy(
                        src_ref=src,
                        dst_ref=dst.at[d - 1],
                        send_sem=send_sem.at[k, d - 1],
                        recv_sem=recv_sem.at[k, d - 1],
                        device_id=where,
                        device_id_type=MESH,
                    )
                    copy.start()
                    copies.append(copy)
    for copy in copies[: 1 - count]:
        copy.wait()
    total = total_ref[...]
    for d in range(1, count):
        total = total + held_total[d - 1]
    mean = jnp.sum(total, 1, keepdims=True) * (1.0 / pixels_all)
    rows = template_ref.shape[1]
    group = rows // BLOCK_ROWS
    diagonal = lax.broadcasted_iota(jnp.int32, (rows, rows), 0) == lax.broadcasted_iota(
        jnp.int32, (rows, rows), 1
    )
    sky_me = lax.axis_index("sky")

    def weight_from(profile, cell):
        block = lax.broadcasted_iota(jnp.int32, profile.shape, 1) // BLOCK_ROWS
        block = lax.rem(block, group)
        wide = [jnp.where(block == g, profile, 0.0) for g in range(group)]
        wide = jnp.concatenate(wide, 0).astype(jnp.bfloat16)
        cell = jnp.concatenate([cell[g].astype(jnp.float32) for g in range(group)], 0)
        return lax.dot_general(
            wide, cell.astype(jnp.bfloat16), (((0,), (0,)), ((), ())),
            preferred_element_type=jnp.float32,
        )

    weights = weight_from(rows_ref[sky_me], cells_ref[me])
    for d in range(1, count):
        weights = weights + weight_from(held_rows[d - 1], held_cells[d - 1])
    for copy in copies[1 - count :]:
        copy.wait()
    for b in range(bands):
        flux = send_ref[me, b].astype(jnp.float32)
        weight = weights[b * rows : (b + 1) * rows]
        for d in range(1, count):
            flux = flux + held[d - 1, b].astype(jnp.float32)
        prior = jnp.sum(jnp.where(diagonal, prior_ref[b : b + 1], 0.0), 1, keepdims=True)
        columns = pl.ds(pl.multiple_of(epoch * part, LANES), part)
        template = template_ref[b, :, columns].astype(jnp.float32)
        depth = weight + prior
        coadd_ref[b] = ((flux + prior * template) / depth).astype(jnp.bfloat16)
        depth_ref[b] = (depth / mean[b : b + 1]).astype(jnp.bfloat16)


def on_device(
    slot_pixels, slot_tile, slot_offset, slot_frac, slot_sigma, clip_mask, slot_count, template, prior_weight
):
    sky = lax.axis_size("sky")
    epochs = lax.axis_size("epoch")
    count = sky * epochs
    slots, bands, rows, cols = slot_pixels.shape
    canvas = rows + 2 * MARGIN
    part = cols // epochs
    vmem = pl.BlockSpec(memory_space=pltpu.VMEM)
    smem = pl.BlockSpec(memory_space=pltpu.SMEM)
    templates = pl.pallas_call(
        functools.partial(gather_kernel, sky),
        out_shape=jax.ShapeDtypeStruct((sky,) + template.shape, jnp.bfloat16),
        in_specs=[vmem],
        out_specs=vmem,
        scratch_shapes=[
            pltpu.VMEM((sky - 1,) + template.shape, jnp.bfloat16),
            pltpu.SemaphoreType.DMA((sky - 1,)),
            pltpu.SemaphoreType.DMA((sky - 1,)),
        ],
        compiler_params=pltpu.CompilerParams(collective_id=0, has_side_effects=True),
        name="gather_templates",
    )(template)
    taps = tap_weights(slot_frac.T).reshape(4 * REACH, slots)
    sigma = slot_sigma.T.astype(jnp.float32)
    scale = CLIP_WIDTH * sigma
    params = jnp.concatenate([taps, scale, 1.0 / scale, 1.0 / (sigma * sigma)], 0)
    patch = sky * rows + 2 * MARGIN
    sums = pltpu.VMEM((bands, patch, cols), jnp.float32)
    held_slots = slots + -slots % 8
    lanes = bands * rows + -(bands * rows) % LANES
    group = rows // BLOCK_ROWS
    patch_blocks = sky * group + 2 * MARGIN // BLOCK_ROWS
    send, total, row_factor, cell_factor = pl.pallas_call(
        functools.partial(warp_kernel, bands, sky, epochs, rows),
        out_shape=(
            jax.ShapeDtypeStruct((count, bands, rows, part), jnp.bfloat16),
            jax.ShapeDtypeStruct((8 * -(-bands // 8), LANES), jnp.float32),
            jax.ShapeDtypeStruct((sky, held_slots, lanes), jnp.float32),
            jax.ShapeDtypeStruct((count, group, held_slots, part), CELL_TYPE),
        ),
        in_specs=[smem] * 4 + [vmem] * 4,
        out_specs=(vmem,) * 4,
        scratch_shapes=[
            sums,
            sums,
            pltpu.VMEM((patch_blocks, held_slots, cols), jnp.float32),
            pltpu.VMEM((bands * rows + 8, cols + LANES), jnp.float32),
        ],
        name="warp_slots",
    )(
        slot_tile[:, 0], slot_offset.T, slot_count, params,
        slot_pixels.reshape(slots, bands * rows, cols), clip_mask, templates, prior_weight,
    )
    block = jax.ShapeDtypeStruct((bands, rows, part), jnp.bfloat16)
    return pl.pallas_call(
        functools.partial(exchange_kernel, bands, sky, epochs, sky * rows * cols),
        out_shape=(block, block),
        in_specs=[vmem] * 6,
        out_specs=(vmem, vmem),
        scratch_shapes=[
            pltpu.VMEM((count - 1,) + send.shape[1:], jnp.bfloat16),
            pltpu.VMEM((count - 1,) + total.shape, jnp.float32),
            pltpu.VMEM((count - 1,) + row_factor.shape[1:], jnp.float32),
            pltpu.VMEM((count - 1,) + cell_factor.shape[1:], CELL_TYPE),
            pltpu.SemaphoreType.DMA((4, count - 1)),
            pltpu.SemaphoreType.DMA((4, count - 1)),
        ],
        compiler_params=pltpu.CompilerParams(collective_id=1, has_side_effects=True),
        name="exchange_sums",
    )(send, total, row_factor, cell_factor, template, prior_weight)


def solution(mesh):
    in_specs = (
        P(("groups", "sky", "epoch"), "band", None, None),
        P(("groups", "sky", "epoch"), None),
        P(("groups", "sky", "epoch"), None),
        P(("groups", "sky", "epoch"), None),
        P(("groups", "sky", "epoch"), "band"),
        P(("groups", "sky", "epoch"), None, None),
        P(("groups", "sky", "epoch")),
        P("band", ("groups", "sky"), None),
        P("band", ("groups", "sky")),
    )
    out_specs = (P("band", ("groups", "sky"), "epoch"), P("band", ("groups", "sky"), "epoch"))
    return jax.shard_map(
        on_device, mesh=mesh, in_specs=in_specs, out_specs=out_specs, check_vma=False
    )
```
